32 devices in a mesh: chan: 4 (over x, core), slab: 8 (over z, y).
Axes of the slice: x: 2, y: 2, z: 4, core: 2. Of those that a mesh axis runs over, the one named last changes fastest.
Arguments:
- beam_images: float32 [64, 512, 4096], P('chan', 'slab'), may hold values from -24 to 24
- chan_weights: int32 [64], P('chan'), may hold values from 1 to 8
- freq_offsets: float32 [64], P('chan'), may hold values from -1 to 1
- half_widths: int32 [5], replicated, may hold values from 16 to 32, as said below
Outputs:
- smoothed: float32 [5, 512, 4096], P(None, 'slab', 'chan')
The draws below stay inside these ranges and needn't reach their ends.
Inputs may be any that keep to these rules, and one draw needn't show every extreme that they name: `half_widths`: each half-width is at least 16 and at most 32; at least one equals 32.
All inputs are finite; a program needn't handle non-finite values.
Results may differ from the reference program's by a relative error of at most 0.00008.
Values sent between devices are 32-bit elements; how exact they have to be, the bound alone decides.
No kernel may reach another device: no remote copies, remote signals or barrier semaphores. Data moves between devices by JAX's collectives and lax.ppermute only.
A program may use at most 128 MiB of HBM per device.

```python
import jax
import jax.numpy as jnp
from jax import lax

NCHAN = 64
NCOLS = 4096
MOMENTS = 5
HW_MAX = 32
NROWS = 512


def draw_half_widths(key, part):
    first_key, second_key = jax.random.split(jax.random.fold_in(key, 17))
    values = jax.random.randint(first_key, (MOMENTS,), HW_MAX // 2, HW_MAX + 1)
    chosen = jax.random.randint(second_key, (), 0, MOMENTS)
    return jnp.where(jnp.arange(MOMENTS) == chosen, HW_MAX, values).astype(jnp.int32)


def with_ends(array, stream_key, low, largest):
    dims = array.shape
    spot = [jax.random.randint(jax.random.fold_in(stream_key, axis), (), 0, dims[axis]) for axis in range(len(dims))]
    array = array.at[tuple(spot)].set(low)
    longest = dims.index(max(dims))
    spot[longest] = (spot[longest] + 1) % dims[longest]
    return array.at[tuple(spot)].set(largest)


def block_scale(stream_key, extent, cuts, smallest, largest):
    gain, own = 1.0, jax.random.fold_in(stream_key, 6)
    for axis_at, blocks in cuts:
        heights = jnp.exp(jax.random.uniform(jax.random.fold_in(own, axis_at), (blocks,), jnp.float32, smallest / len(cuts), largest / len(cuts)))
        gain = gain * jnp.repeat(heights, extent[axis_at] // blocks).reshape([-1 if axis == axis_at else 1 for axis in range(len(extent))])
    return gain


def gaussian(own_key, extent, deviation, bound, pieces=(), dtype=jnp.bfloat16):
    result = jax.random.normal(own_key, extent, jnp.float32) * deviation
    if len(pieces) > 0:
        result = block_scale(own_key, extent, pieces, -0.22, 0.18) * result
    return jnp.clip(result, min=-bound, max=bound).astype(dtype)


def setup_inputs(seed: int = 0) -> dict:
    streams_of = jax.random.split(jax.random.key(seed), 5)
    return {
        "beam_images": gaussian(streams_of[0], (NCHAN, NROWS, NCOLS), 4.0, 24.0, ((0, 4), (1, 8)), jnp.float32),
        "chan_weights": with_ends(jax.random.randint(streams_of[1], (NCHAN,), 1, 9), jax.random.fold_in(streams_of[1], 1), 1, 8).astype(jnp.int32),
        "freq_offsets": jnp.clip(jax.random.uniform(streams_of[2], (NCHAN,), jnp.float32, -1.0, 1.0) * block_scale(streams_of[2], (NCHAN,), ((0, 4),), -0.4, 0.0), -1.0, 1.0),
        "half_widths": draw_half_widths(jax.random.fold_in(streams_of[4], 71), 0),
    }


def window_sum(values, reach, along):
    length = values.shape[along]
    widths = [(0, 0)] * values.ndim
    widths[along] = (HW_MAX + 1, HW_MAX)
    padded = jnp.pad(values, widths)
    running = jnp.cumsum(padded, axis=along)
    upper = lax.dynamic_slice_in_dim(running, (HW_MAX + 1 + reach).astype(jnp.int32), length, along)
    lower = lax.dynamic_slice_in_dim(running, (HW_MAX - reach).astype(jnp.int32), length, along)
    return upper - lower


def reference(beam_images, chan_weights, freq_offsets, half_widths):
    weight_floats = chan_weights.astype(jnp.float32)
    weight_total = jnp.sum(weight_floats)
    powers = jnp.stack([freq_offsets ** power for power in range(MOMENTS)])
    coefficients = powers * weight_floats[None, :] / weight_total
    flat = beam_images.reshape(NCHAN, NROWS * NCOLS)
    moments = jnp.dot(coefficients, flat, precision=lax.Precision.HIGHEST, preferred_element_type=jnp.float32)
    moments = moments.reshape(MOMENTS, NROWS, NCOLS)
    results = []
    for power in range(MOMENTS):
        reach = half_widths[power]
        summed = window_sum(window_sum(moments[power], reach, 0), reach, 1)
        results.append(summed / (2 * reach + 1).astype(jnp.float32))
    return jnp.stack(results)
```

```python
import jax
import jax.numpy as jnp
from jax import lax
from jax.experimental import pallas as pl
from jax.experimental.pallas import tpu as pltpu
from jax.sharding import PartitionSpec as P

MOMENTS = 5
HW_MAX = 32
LANES = 128
BLOCK = 256
TILE = 512
CHUNK = 16


def split(values):
    high = values.astype(jnp.bfloat16)
    low = (values - high.astype(jnp.float32)).astype(jnp.bfloat16)
    return high, low


def moments_kernel(place, weights, offsets, half_widths, images, give, own, total, cells, shots, arrivals, *, groups):
    chans, rows, cols = cells.shape
    owners = 2 * groups
    span = cols // owners
    first_row = pl.multiple_of(place[0], CHUNK)
    copies = [
        pltpu.make_async_copy(
            images.at[:, pl.ds(first_row, rows), pl.ds(part * span, span)],
            cells.at[:, :, pl.ds(part * span, span)],
            arrivals.at[part],
        )
        for part in range(owners)
    ]
    for copy in copies:
        copy.start()
    floats = [weights[chan].astype(jnp.float32) for chan in range(chans)]
    shifts = [offsets[chan] for chan in range(chans)]
    weight_sum = floats[0]
    for value in floats[1:]:
        weight_sum = weight_sum + value
    total[...] = jnp.full(total.shape, weight_sum, jnp.float32)
    edge = jnp.zeros((MOMENTS, rows, LANES), jnp.float32)
    shots[:, :, 0:LANES] = edge
    shots[:, :, LANES + cols : 2 * LANES + cols] = edge
    for part in range(owners):
        copies[part].wait()
        for row in range(0, rows, 8):

            def tile(step, carry):
                at = pl.multiple_of(part * span + step * TILE, TILE)
                sums = [jnp.zeros((8, TILE), jnp.float32)] * MOMENTS
                for chan in range(chans):
                    term = cells[chan, row : row + 8, pl.ds(at, TILE)] * floats[chan]
                    sums[0] = sums[0] + term
                    for power in range(1, MOMENTS):
                        term = term * shifts[chan]
                        sums[power] = sums[power] + term
                for power in range(MOMENTS):
                    shots[power, row : row + 8, pl.ds(LANES + at, TILE)] = sums[power]
                return carry

            lax.fori_loop(0, span // TILE, tile, 0)
    in_main = lax.broadcasted_iota(jnp.int32, (BLOCK, BLOCK), 0)
    out_main = lax.broadcasted_iota(jnp.int32, (BLOCK, BLOCK), 1)
    far_main = jnp.abs(in_main - out_main)
    in_edge = lax.broadcasted_iota(jnp.int32, (LANES, BLOCK), 0)
    in_edge = jnp.where(in_edge < LANES // 2, in_edge + BLOCK, in_edge - LANES)
    far_edge = jnp.abs(in_edge - lax.broadcasted_iota(jnp.int32, (LANES, BLOCK), 1))
    lane = lax.broadcasted_iota(jnp.int32, (rows, LANES), 1)
    for power in range(MOMENTS):
        reach = half_widths[power]
        main_band = (far_main <= reach).astype(jnp.float32).astype(jnp.bfloat16)
        edge_band = (far_edge <= reach).astype(jnp.float32).astype(jnp.bfloat16)
        mains, edges = [], []
        for slot in range(owners):
            start = pl.multiple_of(LANES + place[1 + slot] * span, LANES)
            for at in range(0, span, BLOCK):
                mains.append(shots[power, :, pl.ds(start + at, BLOCK)])
                left = shots[power, :, pl.ds(start + at - LANES, LANES)]
                right = shots[power, :, pl.ds(start + at + BLOCK, LANES)]
                edges.append(jnp.where(lane < LANES // 2, right, left))
        main_high, main_low = split(jnp.concatenate(mains, axis=0))
        edge_high, edge_low = split(jnp.concatenate(edges, axis=0))
        result = jnp.dot(main_high, main_band, preferred_element_type=jnp.float32)
        result = result + jnp.dot(main_low, main_band, preferred_element_type=jnp.float32)
        result = result + jnp.dot(
            jnp.concatenate([edge_high, edge_low], axis=1),
            jnp.concatenate([edge_band, edge_band], axis=0),
            preferred_element_type=jnp.float32,
        )
        count = 0
        for slot in range(owners):
            target = give if slot < groups else own
            for at in range(0, span, BLOCK):
                target[slot % groups, power, :, at : at + BLOCK] = result[count * rows : (count + 1) * rows]
                count += 1


def moments_of(place, chan_weights, freq_offsets, half_widths, beam_images, groups):
    chans, _, cols = beam_images.shape
    span = cols // (2 * groups)
    smem = pl.BlockSpec(memory_space=pltpu.SMEM)
    piece = jax.ShapeDtypeStruct((groups, MOMENTS, CHUNK, span), jnp.float32)
    return pl.pallas_call(
        lambda *refs: moments_kernel(*refs, groups=groups),
        in_specs=[smem, smem, smem, smem, pl.BlockSpec(memory_space=pl.ANY)],
        out_shape=(piece, piece, jax.ShapeDtypeStruct((8, LANES), jnp.float32)),
        scratch_shapes=[
            pltpu.VMEM((chans, CHUNK, cols), jnp.float32),
            pltpu.VMEM((MOMENTS, CHUNK, cols + 2 * LANES), jnp.float32),
            pltpu.SemaphoreType.DMA((2 * groups,)),
        ],
        cost_estimate=pl.CostEstimate(
            flops=20 * chans * CHUNK * cols, bytes_accessed=4 * chans * CHUNK * cols, transcendentals=0
        ),
        name="moments",
    )(place, chan_weights, freq_offsets, half_widths, beam_images)


def rows_kernel(place, half_widths, total, *refs):
    *pieces, out = refs
    rows = out.shape[1]
    depth = rows + 2 * HW_MAX
    out_row = lax.broadcasted_iota(jnp.int32, (rows, depth), 0) + HW_MAX
    stacked = lax.broadcasted_iota(jnp.int32, (rows, depth), 1)
    block = stacked // HW_MAX
    flipped = (depth // HW_MAX - 1 - block) * HW_MAX + (stacked - block * HW_MAX)
    distance = jnp.abs(jnp.where(place[0] == 0, stacked, flipped) - out_row)
    for power in range(MOMENTS):
        reach = half_widths[power]
        band = (distance <= reach).astype(jnp.float32).astype(jnp.bfloat16)
        high, low = split(jnp.concatenate([piece[power] for piece in pieces], axis=0))
        result = jnp.dot(
            jnp.concatenate([band, band], axis=1),
            jnp.concatenate([high, low], axis=0),
            preferred_element_type=jnp.float32,
        )
        divisor = total[...] * (2 * reach + 1).astype(jnp.float32)
        scale = (1.0 / divisor)[0:1, 0:1]
        out[power] = result * scale


def body(beam_images, chan_weights, freq_offsets, half_widths):
    _, slab_rows, all_cols = beam_images.shape
    chan_count = lax.axis_size("chan")
    slab_count = lax.axis_size("slab")
    groups = chan_count // 2
    span = all_cols // chan_count
    mine = lax.axis_index("chan")
    odd = lax.axis_index("slab") % 2
    group, core = mine // 2, mine % 2
    offsets = list(range(1, groups)) + [0]
    slots = [2 * ((group + step) % groups) + side for side in (1 - core, core) for step in offsets]
    swap = [(i, i ^ 1) for i in range(chan_count)]
    near = [(i, i ^ 1) for i in range(slab_count) if i ^ 1 < slab_count]
    far = [(i, ((i + 1) ^ 1) - 1) for i in range(1, slab_count) if ((i + 1) ^ 1) - 1 < slab_count]
    halves = {"far": odd * (slab_rows - HW_MAX), "near": (1 - odd) * (slab_rows - HW_MAX)}
    held, arrived = {"far": [], "near": []}, {"far": [], "near": []}
    for half in ("far", "near"):
        for at in range(0, HW_MAX, CHUNK):
            place = jnp.stack([halves[half] + at] + slots).astype(jnp.int32)
            give, own, total = moments_of(place, chan_weights, freq_offsets, half_widths, beam_images, groups)
            got = lax.ppermute(give, "chan", swap)
            kept = own[groups - 1] + got[groups - 1]
            for order, step in enumerate(offsets[:-1]):
                sent = own[order] + got[order]
                hop = [(i, (i + 2 * step) % chan_count) for i in range(chan_count)]
                kept = kept + lax.ppermute(sent, "chan", hop)
            held[half].append(kept)
            arrived[half].append(lax.ppermute(kept, "slab", far if half == "far" else near))
    total = total + lax.ppermute(total, "chan", swap)
    passed = total
    for step in offsets[:-1]:
        hop = [(i, (i + 2 * step) % chan_count) for i in range(chan_count)]
        total = total + lax.ppermute(passed, "chan", hop)
    pieces = arrived["far"] + held["far"] + held["near"] + arrived["near"]
    smem = pl.BlockSpec(memory_space=pltpu.SMEM)
    vmem = pl.BlockSpec(memory_space=pltpu.VMEM)
    return pl.pallas_call(
        rows_kernel,
        in_specs=[smem, smem, vmem] + [vmem] * len(pieces),
        out_specs=vmem,
        out_shape=jax.ShapeDtypeStruct((MOMENTS, slab_rows, span), jnp.float32),
        name="row_pass",
    )(odd.reshape(1).astype(jnp.int32), half_widths, total, *pieces)


def solution(mesh):
    placed = (P("chan", "slab", None), P("chan"), P("chan"), P())
    return jax.shard_map(
        body, mesh=mesh, in_specs=placed, out_specs=P(None, "slab", "chan"), check_vma=False
    )
```

```python
import jax
import jax.numpy as jnp
from jax import lax
from jax.experimental import pallas as pl
from jax.experimental.pallas import tpu as pltpu
from jax.sharding import PartitionSpec as P


MOMENTS = 5
LANES = 128
BLOCK = 256
ROWS = 8
PARTS = 2

CALLS = (((('far', 0), ('far', 8)), ((0, 2, 0, 5),)), ((('near', 0), ('near', 8)), ((0, 2, 0, 5),)), ((('near', 16), ('near', 24)), ((0, 2, 0, 5),)), ((('far', 16), ('far', 24)), ((0, 2, 0, 4), (0, 2, 4, 5))))


def steps_of(groups):
    return list(range(1, groups)) + [0]


def split(values):
    high = values.astype(jnp.bfloat16)
    low = (values - high.astype(jnp.float32)).astype(jnp.bfloat16)
    return high, low


def moments_kernel(sources, images, *refs, bands, pieces):
    outs, shots = refs[: -4 - len(bands)], refs[-len(bands) :]
    values, cells, bars, arrivals = refs[-4 - len(bands) : -len(bands)]
    _, chans, rows, cols = cells.shape
    groups = outs[0].shape[0] + 1
    owners = 2 * groups
    span = cols // owners
    wide = cols // PARTS
    mine = lax.axis_index("chan")
    odd = lax.axis_index("slab") % 2
    copies = []
    for band, (half, at) in enumerate(bands):
        below = odd if half == "far" else 1 - odd
        first_row = pl.multiple_of(jnp.where(below == 1, images.shape[1] - ROWS - at, at), ROWS)
        for lane_at in range(0, cols, wide):
            copies.append(
                pltpu.make_async_copy(
                    images.at[:, pl.ds(first_row, rows), pl.ds(lane_at, wide)],
                    cells.at[band, :, :, pl.ds(lane_at, wide)],
                    arrivals.at[len(copies)],
                )
            )
    for copy in copies:
        copy.start()
    load = pltpu.make_async_copy(sources, values, arrivals.at[len(copies)])
    load.start()
    load.wait()
    group, core = mine // 2, mine % 2
    slots = [
        2 * ((group + step) % groups) + side for side in (1 - core, core) for step in steps_of(groups)
    ]
    if len(outs) > 4 * len(pieces):
        weight_sum = values[0]
        for chan in range(1, chans):
            weight_sum = weight_sum + values[chan]
        outs[-1][...] = jnp.full(outs[-1].shape, weight_sum, jnp.float32)
    edge = jnp.zeros((MOMENTS, rows, LANES), jnp.float32)
    for shot in shots:
        shot[:, :, 0:LANES] = edge
        shot[:, :, LANES + cols : 2 * LANES + cols] = edge
    depth = rows * chans
    row_at = lax.broadcasted_iota(jnp.int32, (rows, depth), 0)
    col_at = lax.broadcasted_iota(jnp.int32, (rows, depth), 1)
    same_row = col_at % rows == row_at
    weight = jnp.zeros((rows, depth), jnp.float32)
    shift = jnp.zeros((rows, depth), jnp.float32)
    for chan in range(chans):
        here = same_row & (col_at // rows == chan)
        weight = jnp.where(here, values[chan], weight)
        shift = jnp.where(here, values[chans + chan], shift)
    terms = [weight]
    for _ in range(1, MOMENTS):
        terms.append(terms[-1] * shift)
    high, low = split(jnp.concatenate(terms, axis=0))
    mixer = jnp.concatenate(
        [
            jnp.concatenate([high, high], axis=1).astype(jnp.float32),
            jnp.concatenate([low, jnp.zeros_like(low)], axis=1).astype(jnp.float32),
        ],
        axis=0,
    ).astype(jnp.bfloat16)
    in_at = lax.broadcasted_iota(jnp.int32, (BLOCK + LANES, BLOCK), 0)
    in_at = jnp.where(
        in_at < BLOCK + LANES // 2, in_at, jnp.where(in_at < BLOCK, in_at, in_at - BLOCK - LANES)
    )
    distance = jnp.abs(in_at - lax.broadcasted_iota(jnp.int32, (BLOCK + LANES, BLOCK), 1))
    for power in range(MOMENTS):
        reach = values[2 * chans + power].astype(jnp.int32)
        bars[power] = (distance <= reach).astype(jnp.float32).astype(jnp.bfloat16)
    lane = lax.broadcasted_iota(jnp.int32, (rows, LANES), 1)

    def mix(band, lane_at):
        stack = cells[band, :, :, lane_at : lane_at + BLOCK].reshape(depth, BLOCK)
        mixed = jnp.dot(mixer, jnp.concatenate(split(stack), axis=0), preferred_element_type=jnp.float32)
        mixed = mixed[: rows * MOMENTS] + mixed[rows * MOMENTS :]
        shots[band][:, :, LANES + lane_at : LANES + lane_at + BLOCK] = mixed.reshape(MOMENTS, rows, BLOCK)

    def smooth(band, power):
        mains, edges = [], []
        for slot in range(owners):
            start = pl.multiple_of(LANES + slots[slot] * span, LANES)
            for lane_at in range(0, span, BLOCK):
                mains.append(shots[band][power, :, pl.ds(start + lane_at, BLOCK)])
                left = shots[band][power, :, pl.ds(start + lane_at - LANES, LANES)]
                right = shots[band][power, :, pl.ds(start + lane_at + BLOCK, LANES)]
                edges.append(jnp.where(lane < LANES // 2, right, left))
        main_high, main_low = split(jnp.concatenate(mains, axis=0))
        edge_high, edge_low = split(jnp.concatenate(edges, axis=0))
        main_bar, edge_bar = bars[power, :BLOCK], bars[power, BLOCK:]
        result = jnp.dot(main_high, main_bar, preferred_element_type=jnp.float32)
        result = result + jnp.dot(main_low, main_bar, preferred_element_type=jnp.float32)
        result = result + jnp.dot(
            jnp.concatenate([edge_high, edge_low], axis=1),
            jnp.concatenate([edge_bar, edge_bar], axis=0),
            preferred_element_type=jnp.float32,
        )
        result = result.reshape(owners, span // BLOCK, rows, BLOCK)
        for index, (first, size, low_power, high_power) in enumerate(pieces):
            if not (first <= band < first + size and low_power <= power < high_power):
                continue
            row = (band - first) * rows
            for slot in range(owners):
                order = slot % groups
                target = outs[4 * index + 2 * (slot >= groups) + (order == groups - 1)]
                for block in range(span // BLOCK):
                    target[
                        order % (groups - 1),
                        power - low_power,
                        row : row + rows,
                        block * BLOCK : (block + 1) * BLOCK,
                    ] = result[slot, block]

    for band in range(len(bands)):
        ready = [(band - 1, power) for power in range(MOMENTS)] if band > 0 else []
        for part in range(PARTS):
            copies[PARTS * band + part].wait()
            work = [(part * wide + at) for at in range(0, wide, BLOCK)]
            share = ready[part * MOMENTS // PARTS : (part + 1) * MOMENTS // PARTS]
            for index, lane_at in enumerate(work):
                mix(band, lane_at)
                if index % 2 == 1 and share:
                    smooth(*share.pop(0))
            for item in share:
                smooth(*item)
    for power in range(MOMENTS):
        smooth(len(bands) - 1, power)


def moments_of(values, beam_images, groups, bands, pieces, weigh):
    chans, _, cols = beam_images.shape
    span = cols // (2 * groups)
    outs = []
    for _, size, low_power, high_power in pieces:
        for count in (groups - 1, 1) * 2:
            shape = (count, high_power - low_power, size * ROWS, span)
            outs.append(jax.ShapeDtypeStruct(shape, jnp.float32))
    if weigh:
        outs.append(jax.ShapeDtypeStruct((8, LANES), jnp.float32))
    work = len(bands) * ROWS * chans * cols
    return pl.pallas_call(
        lambda *refs: moments_kernel(*refs, bands=bands, pieces=pieces),
        in_specs=[pl.BlockSpec(memory_space=pl.ANY), pl.BlockSpec(memory_space=pl.ANY)],
        out_shape=tuple(outs),
        scratch_shapes=[
            pltpu.SMEM(values.shape, jnp.float32),
            pltpu.VMEM((len(bands), chans, ROWS, cols), jnp.float32),
            pltpu.VMEM((MOMENTS, BLOCK + LANES, BLOCK), jnp.bfloat16),
            pltpu.SemaphoreType.DMA((PARTS * len(bands) + 1,)),
            *[pltpu.VMEM((MOMENTS, ROWS, cols + 2 * LANES), jnp.float32) for _ in bands],
        ],
        cost_estimate=pl.CostEstimate(flops=20 * work, bytes_accessed=4 * work, transcendentals=0),
        compiler_params=pltpu.CompilerParams(vmem_limit_bytes=48 * 2**20),
        name="moments",
    )(values, beam_images)


def window(shape, groups, first_row, slab_rows, odd):
    out_row = lax.broadcasted_iota(jnp.int32, shape, 0) + first_row
    stacked = lax.broadcasted_iota(jnp.int32, shape, 1)
    place = jnp.zeros(shape, jnp.int32)
    for index, (half, at, mine) in enumerate(groups):
        below = odd if half == "far" else 1 - odd
        lower = slab_rows - ROWS - at if mine else slab_rows + at
        upper = at if mine else -ROWS - at
        start = jnp.where(below == 1, lower, upper) - index * ROWS
        place = jnp.where(stacked // ROWS == index, stacked + start, place)
    return jnp.abs(place - out_row)


def banded(distance, reach, rows):
    bar = (distance <= reach).astype(jnp.float32).astype(jnp.bfloat16)
    high, low = split(rows)
    return jnp.dot(bar, high, preferred_element_type=jnp.float32) + jnp.dot(
        bar, low, preferred_element_type=jnp.float32
    )


def scale_of(total, reach):
    return (1.0 / (total[...] * (2 * reach + 1).astype(jnp.float32)))[0:1, 0:1]


def inner_kernel(values, total, *refs, chans, groups, half, bounds):
    *pieces, out, rest = refs
    odd = lax.axis_index("slab") % 2
    below = odd if half == "far" else 1 - odd
    rows, late = out.shape[1], rest.shape[1]
    distance = window((rows, ROWS * len(groups)), groups, 0, rows, odd)
    for power in range(MOMENTS):
        reach = values[2 * chans + power].astype(jnp.int32)
        parts = [
            piece[power - low]
            for piece, low in zip(pieces, bounds)
            if low <= power < low + piece.shape[0]
        ]
        result = banded(distance, reach, jnp.concatenate(parts, axis=0))
        out[power] = result * scale_of(total, reach)
        rest[power] = jnp.where(below == 1, result[rows - late :], result[:late])


def edge_kernel(values, total, rest, *refs, chans, groups, starts):
    *lasts, _, out, edge, sent = refs
    odd = lax.axis_index("slab") % 2
    slab_rows, late = out.shape[1], rest.shape[1]
    below = odd if groups[0][0] == "far" else 1 - odd
    first_row = pl.multiple_of(jnp.where(below == 1, slab_rows - late, 0), ROWS)
    distance = window((late, ROWS * len(groups)), groups, first_row, slab_rows, odd)
    copies = []
    for power in range(MOMENTS):
        reach = values[2 * chans + power].astype(jnp.int32)
        index = max(index for index, start in enumerate(starts) if start <= power)
        last = lasts[index][power - starts[index]]
        edge[power] = (rest[power] + banded(distance, reach, last)) * scale_of(total, reach)
        copies.append(
            pltpu.make_async_copy(edge.at[power], out.at[power, pl.ds(first_row, late), :], sent.at[power])
        )
        copies[-1].start()
    for copy in copies:
        copy.wait()


def body(beam_images, chan_weights, freq_offsets, half_widths):
    chans, slab_rows, all_cols = beam_images.shape
    chan_count = lax.axis_size("chan")
    slab_count = lax.axis_size("slab")
    groups = chan_count // 2
    span = all_cols // chan_count
    extent = 2 * chans + MOMENTS
    slot = jnp.arange(extent)
    spread = [
        jnp.pad(part, (before, extent - before - part.shape[0]))
        for part, before in ((chan_weights, 0), (half_widths, 2 * chans), (freq_offsets, chans))
    ]
    values = jnp.where(slot // chans == 1, spread[2], (spread[0] + spread[1]).astype(jnp.float32))
    steps = steps_of(groups)
    hops = [[(i, (i + 2 * step) % chan_count) for i in range(chan_count)] for step in steps[:-1]]
    swap = [(i, i ^ 1) for i in range(chan_count)]
    pairs = {
        "near": [(i, i ^ 1) for i in range(slab_count) if i ^ 1 < slab_count],
        "far": [(i, ((i + 1) ^ 1) - 1) for i in range(1, slab_count) if ((i + 1) ^ 1) - 1 < slab_count],
    }
    held, arrived, covers = [], [], []
    for call, (bands, pieces) in enumerate(CALLS):
        outs = moments_of(values, beam_images, groups, bands, pieces, call == len(CALLS) - 1)
        for index, (first, size, low, high) in enumerate(pieces):
            give, give_kept, own, own_kept = outs[4 * index : 4 * index + 4]
            got = lax.ppermute(give, "chan", swap)
            got_kept = lax.ppermute(give_kept, "chan", swap)
            kept = own_kept[0] + got_kept[0]
            for order, hop in enumerate(hops):
                sent = own[order] + got[order]
                came = lax.ppermute(sent, "chan", hop)
                kept = kept + came
            held.append(kept)
            half = bands[first][0]
            covers.append((bands[first : first + size], low))
            arrived.append(lax.ppermute(kept, "slab", pairs[half]))
    total = outs[-1]
    total = total + lax.ppermute(total, "chan", swap)
    passed = total
    for hop in hops:
        total = total + lax.ppermute(passed, "chan", hop)
    smem = pl.BlockSpec(memory_space=pltpu.SMEM)
    vmem = pl.BlockSpec(memory_space=pltpu.VMEM)
    anywhere = pl.BlockSpec(memory_space=pl.ANY)
    last = len(CALLS[-1][1])
    pieces = held + arrived[:-last]
    groups = [(*band, True, low) for cover, low in covers for band in cover]
    groups += [(*band, False, low) for cover, low in covers[:-last] for band in cover]
    groups = [group[:3] for group in groups if group[3] == 0]
    bounds = [low for _, low in covers] + [low for _, low in covers[:-last]]
    starts = [low for _, low in covers[-last:]]
    edges = covers[-1][0]
    late = len(edges) * ROWS
    shape = jax.ShapeDtypeStruct((MOMENTS, slab_rows, span), jnp.float32)
    result, rest = pl.pallas_call(
        lambda *refs: inner_kernel(
            *refs, chans=chans, groups=groups, half=edges[0][0], bounds=bounds
        ),
        in_specs=[smem, vmem] + [vmem] * len(pieces),
        out_specs=(vmem, vmem),
        out_shape=(shape, jax.ShapeDtypeStruct((MOMENTS, late, span), jnp.float32)),
        compiler_params=pltpu.CompilerParams(vmem_limit_bytes=16 * 2**20),
        name="inner_rows",
    )(values, total, *pieces)
    return pl.pallas_call(
        lambda *refs: edge_kernel(
            *refs, chans=chans, groups=[(*band, False) for band in edges], starts=starts
        ),
        in_specs=[smem, vmem, vmem] + [vmem] * last + [anywhere],
        out_specs=anywhere,
        out_shape=shape,
        scratch_shapes=[
            pltpu.VMEM((MOMENTS, late, span), jnp.float32),
            pltpu.SemaphoreType.DMA((MOMENTS,)),
        ],
        input_output_aliases={3 + last: 0},
        compiler_params=pltpu.CompilerParams(vmem_limit_bytes=16 * 2**20),
        name="edge_rows",
    )(values, total, rest, *arrived[-last:], result)


def solution(mesh):
    placed = (P("chan", "slab", None), P("chan"), P("chan"), P())

    return jax.shard_map(body, mesh=mesh, in_specs=placed, out_specs=P(None, "slab", "chan"), check_vma=False)
```

```python
import jax
import jax.numpy as jnp
from jax import lax
from jax.experimental import pallas as pl
from jax.experimental.pallas import tpu as pltpu
from jax.sharding import PartitionSpec as P


MOMENTS = 5
LANES = 128
BLOCK = 256
ROWS = 8
PARTS = 2

CALLS = (((('far', 0), ('far', 8)), ((0, 2, 0, 5),)), ((('near', 0), ('near', 8)), ((0, 2, 0, 5),)), ((('near', 16), ('near', 24)), ((0, 2, 0, 5),)), ((('far', 16), ('far', 24)), ((0, 2, 0, 4), (0, 2, 4, 5))))


def steps_of(groups):
    return list(range(1, groups)) + [0]


def split(values):
    high = values.astype(jnp.bfloat16)
    low = (values - high.astype(jnp.float32)).astype(jnp.bfloat16)
    return high, low


def moments_kernel(sources, images, *refs, bands, pieces):
    outs, shots = refs[: -4 - len(bands)], refs[-len(bands) :]
    values, cells, bars, arrivals = refs[-4 - len(bands) : -len(bands)]
    _, chans, rows, cols = cells.shape
    groups = outs[0].shape[0] + 1
    owners = 2 * groups
    span = cols // owners
    wide = cols // PARTS
    mine = lax.axis_index("chan")
    odd = lax.axis_index("slab") % 2
    copies = []
    for band, (half, at) in enumerate(bands):
        below = odd if half == "far" else 1 - odd
        first_row = pl.multiple_of(jnp.where(below == 1, images.shape[1] - ROWS - at, at), ROWS)
        for lane_at in range(0, cols, wide):
            copies.append(
                pltpu.make_async_copy(
                    images.at[:, pl.ds(first_row, rows), pl.ds(lane_at, wide)],
                    cells.at[band, :, :, pl.ds(lane_at, wide)],
                    arrivals.at[len(copies)],
                )
            )
    for copy in copies:
        copy.start()
    load = pltpu.make_async_copy(sources, values, arrivals.at[len(copies)])
    load.start()
    load.wait()
    group, core = mine // 2, mine % 2
    slots = [
        2 * ((group + step) % groups) + side for side in (1 - core, core) for step in steps_of(groups)
    ]
    if len(outs) > 4 * len(pieces):
        weight_sum = values[0]
        for chan in range(1, chans):
            weight_sum = weight_sum + values[chan]
        outs[-1][...] = jnp.full(outs[-1].shape, weight_sum, jnp.float32)
    edge = jnp.zeros((MOMENTS, rows, LANES), jnp.float32)
    for shot in shots:
        shot[:, :, 0:LANES] = edge
        shot[:, :, LANES + cols : 2 * LANES + cols] = edge
    depth = rows * chans
    row_at = lax.broadcasted_iota(jnp.int32, (rows, depth), 0)
    col_at = lax.broadcasted_iota(jnp.int32, (rows, depth), 1)
    same_row = col_at % rows == row_at
    weight = jnp.zeros((rows, depth), jnp.float32)
    shift = jnp.zeros((rows, depth), jnp.float32)
    for chan in range(chans):
        here = same_row & (col_at // rows == chan)
        weight = jnp.where(here, values[chan], weight)
        shift = jnp.where(here, values[chans + chan], shift)
    terms = [weight]
    for _ in range(1, MOMENTS):
        terms.append(terms[-1] * shift)
    high, low = split(jnp.concatenate(terms, axis=0))
    mixer = jnp.concatenate(
        [
            jnp.concatenate([high, high], axis=1).astype(jnp.float32),
            jnp.concatenate([low, jnp.zeros_like(low)], axis=1).astype(jnp.float32),
        ],
        axis=0,
    ).astype(jnp.bfloat16)
    in_at = lax.broadcasted_iota(jnp.int32, (BLOCK + LANES, BLOCK), 0)
    in_at = jnp.where(
        in_at < BLOCK + LANES // 2, in_at, jnp.where(in_at < BLOCK, in_at, in_at - BLOCK - LANES)
    )
    distance = jnp.abs(in_at - lax.broadcasted_iota(jnp.int32, (BLOCK + LANES, BLOCK), 1))
    for power in range(MOMENTS):
        reach = values[2 * chans + power].astype(jnp.int32)
        bars[power] = (distance <= reach).astype(jnp.float32).astype(jnp.bfloat16)
    lane = lax.broadcasted_iota(jnp.int32, (rows, LANES), 1)

    def mix(band, lane_at):
        stack = cells[band, :, :, lane_at : lane_at + BLOCK].reshape(depth, BLOCK)
        mixed = jnp.dot(mixer, jnp.concatenate(split(stack), axis=0), preferred_element_type=jnp.float32)
        mixed = mixed[: rows * MOMENTS] + mixed[rows * MOMENTS :]
        shots[band][:, :, LANES + lane_at : LANES + lane_at + BLOCK] = mixed.reshape(MOMENTS, rows, BLOCK)

    def smooth(band, power):
        mains, edges = [], []
        for slot in range(owners):
            start = pl.multiple_of(LANES + slots[slot] * span, LANES)
            for lane_at in range(0, span, BLOCK):
                mains.append(shots[band][power, :, pl.ds(start + lane_at, BLOCK)])
                left = shots[band][power, :, pl.ds(start + lane_at - LANES, LANES)]
                right = shots[band][power, :, pl.ds(start + lane_at + BLOCK, LANES)]
                edges.append(jnp.where(lane < LANES // 2, right, left))
        main_high, main_low = split(jnp.concatenate(mains, axis=0))
        edge_high, edge_low = split(jnp.concatenate(edges, axis=0))
        main_bar, edge_bar = bars[power, :BLOCK], bars[power, BLOCK:]
        result = jnp.dot(main_high, main_bar, preferred_element_type=jnp.float32)
        result = result + jnp.dot(main_low, main_bar, preferred_element_type=jnp.float32)
        result = result + jnp.dot(
            jnp.concatenate([edge_high, edge_low], axis=1),
            jnp.concatenate([edge_bar, edge_bar], axis=0),
            preferred_element_type=jnp.float32,
        )
        result = result.reshape(owners, span // BLOCK, rows, BLOCK)
        for index, (first, size, low_power, high_power) in enumerate(pieces):
            if not (first <= band < first + size and low_power <= power < high_power):
                continue
            row = (band - first) * rows
            for slot in range(owners):
                order = slot % groups
                target = outs[4 * index + 2 * (slot >= groups) + (order == groups - 1)]
                for block in range(span // BLOCK):
                    target[
                        order % (groups - 1),
                        power - low_power,
                        row : row + rows,
                        block * BLOCK : (block + 1) * BLOCK,
                    ] = result[slot, block]

    for band in range(len(bands)):
        ready = [(band - 1, power) for power in range(MOMENTS)] if band > 0 else []
        for part in range(PARTS):
            copies[PARTS * band + part].wait()
            work = [(part * wide + at) for at in range(0, wide, BLOCK)]
            share = ready[part * MOMENTS // PARTS : (part + 1) * MOMENTS // PARTS]
            for index, lane_at in enumerate(work):
                mix(band, lane_at)
                if index % 2 == 1 and share:
                    smooth(*share.pop(0))
            for item in share:
                smooth(*item)
    for power in range(MOMENTS):
        smooth(len(bands) - 1, power)


def moments_of(values, beam_images, groups, bands, pieces, weigh):
    chans, _, cols = beam_images.shape
    span = cols // (2 * groups)
    outs = []
    for _, size, low_power, high_power in pieces:
        for count in (groups - 1, 1) * 2:
            shape = (count, high_power - low_power, size * ROWS, span)
            outs.append(jax.ShapeDtypeStruct(shape, jnp.float32))
    if weigh:
        outs.append(jax.ShapeDtypeStruct((8, LANES), jnp.float32))
    work = len(bands) * ROWS * chans * cols
    return pl.pallas_call(
        lambda *refs: moments_kernel(*refs, bands=bands, pieces=pieces),
        in_specs=[pl.BlockSpec(memory_space=pl.ANY), pl.BlockSpec(memory_space=pl.ANY)],
        out_shape=tuple(outs),
        scratch_shapes=[
            pltpu.SMEM(values.shape, jnp.float32),
            pltpu.VMEM((len(bands), chans, ROWS, cols), jnp.float32),
            pltpu.VMEM((MOMENTS, BLOCK + LANES, BLOCK), jnp.bfloat16),
            pltpu.SemaphoreType.DMA((PARTS * len(bands) + 1,)),
            *[pltpu.VMEM((MOMENTS, ROWS, cols + 2 * LANES), jnp.float32) for _ in bands],
        ],
        cost_estimate=pl.CostEstimate(flops=20 * work, bytes_accessed=4 * work, transcendentals=0),
        compiler_params=pltpu.CompilerParams(vmem_limit_bytes=48 * 2**20),
        name="moments",
    )(values, beam_images)


def window(shape, groups, first_row, slab_rows, odd):
    out_row = lax.broadcasted_iota(jnp.int32, shape, 0) + first_row
    stacked = lax.broadcasted_iota(jnp.int32, shape, 1)
    place = jnp.zeros(shape, jnp.int32)
    for index, (half, at, mine) in enumerate(groups):
        below = odd if half == "far" else 1 - odd
        lower = slab_rows - ROWS - at if mine else slab_rows + at
        upper = at if mine else -ROWS - at
        start = jnp.where(below == 1, lower, upper) - index * ROWS
        place = jnp.where(stacked // ROWS == index, stacked + start, place)
    return jnp.abs(place - out_row)


def banded(distance, reach, rows):
    bar = (distance <= reach).astype(jnp.float32).astype(jnp.bfloat16)
    high, low = split(rows)
    return jnp.dot(bar, high, preferred_element_type=jnp.float32) + jnp.dot(
        bar, low, preferred_element_type=jnp.float32
    )


def scale_of(total, reach):
    return (1.0 / (total[...] * (2 * reach + 1).astype(jnp.float32)))[0:1, 0:1]


def inner_kernel(values, total, *refs, chans, groups, half, bounds):
    *pieces, out, rest, marks = refs
    odd = lax.axis_index("slab") % 2
    below = odd if half == "far" else 1 - odd
    rows, late = out.shape[1], rest.shape[1]
    distance = window((rows, ROWS * len(groups)), groups, 0, rows, odd)
    for power in range(MOMENTS):
        reach = values[2 * chans + power].astype(jnp.int32)
        parts = [
            piece[power - low]
            for piece, low in zip(pieces, bounds)
            if low <= power < low + piece.shape[0]
        ]
        result = banded(distance, reach, jnp.concatenate(parts, axis=0))
        scale = scale_of(total, reach)
        marks[power : power + 1] = jnp.full((1, LANES), reach, jnp.int32).astype(jnp.float32)
        marks[ROWS + power : ROWS + power + 1] = jnp.broadcast_to(scale, (1, LANES))
        out[power] = result * scale
        rest[power] = jnp.where(below == 1, result[rows - late :], result[:late])


def edge_kernel(rest, marks, *refs, groups, starts):
    *lasts, _, out, edge, sent = refs
    odd = lax.axis_index("slab") % 2
    slab_rows, late = out.shape[1], rest.shape[1]
    below = odd if groups[0][0] == "far" else 1 - odd
    first_row = pl.multiple_of(jnp.where(below == 1, slab_rows - late, 0), ROWS)
    distance = window((late, ROWS * len(groups)), groups, first_row, slab_rows, odd)
    distance = distance.astype(jnp.float32)
    copies = []
    for power in range(MOMENTS):
        reach = marks[power : power + 1, : distance.shape[1]]
        scale = marks[ROWS + power : ROWS + power + 1, 0:1]
        index = max(index for index, start in enumerate(starts) if start <= power)
        last = lasts[index][power - starts[index]]
        edge[power] = (rest[power] + banded(distance, reach, last)) * scale
        copies.append(
            pltpu.make_async_copy(edge.at[power], out.at[power, pl.ds(first_row, late), :], sent.at[power])
        )
        copies[-1].start()
    for copy in copies:
        copy.wait()


def body(beam_images, chan_weights, freq_offsets, half_widths):
    chans, slab_rows, all_cols = beam_images.shape
    chan_count = lax.axis_size("chan")
    slab_count = lax.axis_size("slab")
    groups = chan_count // 2
    span = all_cols // chan_count
    extent = 2 * chans + MOMENTS
    slot = jnp.arange(extent)
    spread = [
        jnp.pad(part, (before, extent - before - part.shape[0]))
        for part, before in ((chan_weights, 0), (half_widths, 2 * chans), (freq_offsets, chans))
    ]
    values = jnp.where(slot // chans == 1, spread[2], (spread[0] + spread[1]).astype(jnp.float32))
    steps = steps_of(groups)
    hops = [[(i, (i + 2 * step) % chan_count) for i in range(chan_count)] for step in steps[:-1]]
    swap = [(i, i ^ 1) for i in range(chan_count)]
    pairs = {
        "near": [(i, i ^ 1) for i in range(slab_count) if i ^ 1 < slab_count],
        "far": [(i, ((i + 1) ^ 1) - 1) for i in range(1, slab_count) if ((i + 1) ^ 1) - 1 < slab_count],
    }
    held, arrived, covers = [], [], []
    for call, (bands, pieces) in enumerate(CALLS):
        outs = moments_of(values, beam_images, groups, bands, pieces, call == len(CALLS) - 1)
        for index, (first, size, low, high) in enumerate(pieces):
            give, give_kept, own, own_kept = outs[4 * index : 4 * index + 4]
            got = lax.ppermute(give, "chan", swap)
            got_kept = lax.ppermute(give_kept, "chan", swap)
            kept = own_kept[0] + got_kept[0]
            for order, hop in enumerate(hops):
                sent = own[order] + got[order]
                came = lax.ppermute(sent, "chan", hop)
                kept = kept + came
            held.append(kept)
            half = bands[first][0]
            covers.append((bands[first : first + size], low))
            arrived.append(lax.ppermute(kept, "slab", pairs[half]))
    total = outs[-1]
    total = total + lax.ppermute(total, "chan", swap)
    passed = total
    for hop in hops:
        total = total + lax.ppermute(passed, "chan", hop)
    smem = pl.BlockSpec(memory_space=pltpu.SMEM)
    vmem = pl.BlockSpec(memory_space=pltpu.VMEM)
    anywhere = pl.BlockSpec(memory_space=pl.ANY)
    last = len(CALLS[-1][1])
    pieces = held + arrived[:-last]
    groups = [(*band, True, low) for cover, low in covers for band in cover]
    groups += [(*band, False, low) for cover, low in covers[:-last] for band in cover]
    groups = [group[:3] for group in groups if group[3] == 0]
    bounds = [low for _, low in covers] + [low for _, low in covers[:-last]]
    starts = [low for _, low in covers[-last:]]
    edges = covers[-1][0]
    late = len(edges) * ROWS
    shape = jax.ShapeDtypeStruct((MOMENTS, slab_rows, span), jnp.float32)
    result, rest, marks = pl.pallas_call(
        lambda *refs: inner_kernel(
            *refs, chans=chans, groups=groups, half=edges[0][0], bounds=bounds
        ),
        in_specs=[smem, vmem] + [vmem] * len(pieces),
        out_specs=(vmem, vmem, vmem),
        out_shape=(
            shape,
            jax.ShapeDtypeStruct((MOMENTS, late, span), jnp.float32),
            jax.ShapeDtypeStruct((2 * ROWS, LANES), jnp.float32),
        ),
        compiler_params=pltpu.CompilerParams(vmem_limit_bytes=16 * 2**20),
        name="inner_rows",
    )(values, total, *pieces)
    return pl.pallas_call(
        lambda *refs: edge_kernel(
            *refs, groups=[(*band, False) for band in edges], starts=starts
        ),
        in_specs=[vmem, vmem] + [vmem] * last + [anywhere],
        out_specs=anywhere,
        out_shape=shape,
        scratch_shapes=[
            pltpu.VMEM((MOMENTS, late, span), jnp.float32),
            pltpu.SemaphoreType.DMA((MOMENTS,)),
        ],
        input_output_aliases={2 + last: 0},
        compiler_params=pltpu.CompilerParams(vmem_limit_bytes=16 * 2**20),
        name="edge_rows",
    )(rest, marks, *arrived[-last:], result)


def solution(mesh):
    placed = (P("chan", "slab", None), P("chan"), P("chan"), P())

    return jax.shard_map(body, mesh=mesh, in_specs=placed, out_specs=P(None, "slab", "chan"), check_vma=False)
```
